768 devices in a mesh: gx: 8 (over y), gy: 8 (over z_lo, core), gz: 12 (over z_hi, x).
Axes of the slice: x: 4, y: 8, z: 12 (z_hi: 3, z_lo: 4; z = z_hi * 4 + z_lo), core: 2. Of those that a mesh axis runs over, the one named last changes fastest.
Arguments:
- positions: float32 [3, 16, 32, 24, 128], P(None, 'gx', 'gy', 'gz'), may hold values from 0 to 1
- type_ids: int32 [16, 32, 24, 128], P('gx', 'gy', 'gz'), may hold values from 0 to 1
- counts: int32 [16, 32, 24], P('gx', 'gy', 'gz'), may hold values from 64 to 128
- type_charge: float32 [2], replicated, may hold values from -1 to 1
- type_sigma: float32 [2], replicated, may hold values from 0.2 to 0.35
- type_epsilon: float32 [2], replicated, may hold values from 0.05 to 0.5
Outputs:
- forces: float32 [3, 16, 32, 24, 128], P(None, 'gx', 'gy', 'gz')
- totals: float32 [2], replicated
The draws below stay inside these ranges and needn't reach their ends.
All inputs are finite; a program needn't handle non-finite values.
Results may differ from the reference program's by a relative error of at most 0.0003.
Values sent between devices are 32-bit elements; how exact they have to be, the bound alone decides.
No kernel may reach another device: no remote copies, remote signals or barrier semaphores. Data moves between devices by JAX's collectives and lax.ppermute only.
A program may use at most 64 MiB of HBM per device.

```python
import math
import jax
import jax.numpy as jnp
from jax import lax

ATOMS_CELL = 128
TYPES = 2
NX = 16
NY = 32
NZ = 24


def plant(result, stream_key, smallest, top_value):
    dims = result.shape
    spot = [jax.random.randint(jax.random.fold_in(stream_key, axis), (), 0, dims[axis]) for axis in range(len(dims))]
    result = result.at[tuple(spot)].set(smallest)
    longest = dims.index(max(dims))
    spot[longest] = (spot[longest] + 1) % dims[longest]
    return result.at[tuple(spot)].set(top_value)


def block_scale(own_key, shape, split, low, high):
    factor_of = 1.0
    for axis_at, shards_of in split:
        steps = jax.random.uniform(jax.random.fold_in(jax.random.fold_in(own_key, 6), axis_at), (shards_of,), jnp.float32, low / len(split), high / len(split))
        factor_of = factor_of * jnp.repeat(jnp.exp(steps), shape[axis_at] // shards_of).reshape((-1,) + (1,) * (len(shape) - 1 - axis_at))
    return factor_of


def setup_inputs(seed: int = 0) -> dict:
    key_of = jax.random.split(jax.random.key(seed), 7)
    return {
        "positions": jnp.clip(1.0 * jax.random.uniform(key_of[0], (3, NX, NY, NZ, ATOMS_CELL), jnp.float32) ** block_scale(key_of[0], (3, NX, NY, NZ, ATOMS_CELL), ((1, 8), (2, 8), (3, 12)), -0.2, 0.2), 0.0, 1.0),
        "type_ids": plant(jax.random.randint(key_of[1], (NX, NY, NZ, ATOMS_CELL), 0, TYPES), jax.random.fold_in(key_of[1], 1), 0, TYPES - 1).astype(jnp.int32),
        "counts": plant(jax.random.randint(key_of[2], (NX, NY, NZ), ATOMS_CELL // 2, ATOMS_CELL + 1), jax.random.fold_in(key_of[2], 1), ATOMS_CELL // 2, ATOMS_CELL).astype(jnp.int32),
        "type_charge": jnp.clip(jax.random.uniform(key_of[3], (TYPES,), jnp.float32, -1.0, 1.0), -1.0, 1.0),
        "type_sigma": jnp.clip(jnp.exp(jax.random.uniform(key_of[4], (TYPES,), jnp.float32, math.log(0.2), math.log(0.35))), 0.2, 0.35),
        "type_epsilon": jnp.clip(jnp.exp(jax.random.uniform(key_of[5], (TYPES,), jnp.float32, math.log(0.05), math.log(0.5))), 0.05, 0.5),
    }


soft_core = 0.09
corner_pairs = [(first_corner, second_corner) for first_corner in range(8) for second_corner in range(8) if first_corner & second_corner == 0 and first_corner <= second_corner]

def corner_of(which):
    return (which & 1, which >> 1 & 1, which >> 2 & 1)

def atom_table(positions, type_ids, counts, type_charge, type_sigma, type_epsilon):
    type_count = type_charge.shape[0]
    kinds_shape = (type_count, 1, 1, 1, 1)
    onehot = (type_ids[None] == jnp.arange(type_count, dtype=jnp.int32).reshape(kinds_shape)).astype(jnp.float32)
    charge = lax.optimization_barrier(jnp.sum(onehot * type_charge.reshape(kinds_shape), 0))
    sigma_atom = lax.optimization_barrier(jnp.sum(onehot * type_sigma.reshape(kinds_shape), 0))
    depth_atom = lax.optimization_barrier(jnp.sum(onehot * jnp.sqrt(type_epsilon).reshape(kinds_shape), 0))
    slots = lax.broadcasted_iota(jnp.int32, type_ids.shape, 3)
    occupied = (slots < counts[..., None]).astype(jnp.float32)
    return jnp.stack([positions[0], positions[1], positions[2], charge, sigma_atom, depth_atom, occupied])

def pair_terms(first, second, offset, selfpair):
    displace = second[:3, :, None, :] - first[:3, :, :, None] + offset[:, None, None, None]
    dist_sq = lax.optimization_barrier(jnp.sum(displace * displace, 0))
    width_atoms = first.shape[-1]
    live_mask = first[6][:, :, None] * second[6][:, None, :] * (dist_sq < 1.0).astype(jnp.float32)
    if selfpair:
        ordered = (lax.broadcasted_iota(jnp.int32, (width_atoms, width_atoms), 0) < lax.broadcasted_iota(jnp.int32, (width_atoms, width_atoms), 1)).astype(jnp.float32)
        live_mask = live_mask * ordered[None]
    sigma_pair = 0.5 * (first[4][:, :, None] + second[4][:, None, :])
    depth_pair = first[5][:, :, None] * second[5][:, None, :]
    coulomb = first[3][:, :, None] * second[3][:, None, :]
    soft_sq = dist_sq + soft_core
    inverse = lax.rsqrt(soft_sq)
    ratio_six = (sigma_pair * sigma_pair / soft_sq) ** 3
    ratio_twelve = ratio_six * ratio_six
    value_here = 4.0 * depth_pair * (ratio_twelve - ratio_six) + coulomb * inverse
    slope_here = (4.0 * depth_pair * (6.0 * ratio_six - 12.0 * ratio_twelve) - coulomb * inverse) * inverse
    cut_sq = 1.0 + soft_core
    cut_len = cut_sq ** 0.5
    cut_six = (sigma_pair * sigma_pair / cut_sq) ** 3
    cut_twelve = cut_six * cut_six
    value_cut = 4.0 * depth_pair * (cut_twelve - cut_six) + coulomb / cut_len
    slope_cut = (4.0 * depth_pair * (6.0 * cut_six - 12.0 * cut_twelve) - coulomb / cut_len) / cut_len
    energy = live_mask * (value_here - value_cut - (soft_sq * inverse - cut_len) * slope_cut)
    slope = live_mask * (slope_here - slope_cut) * inverse
    weighted = slope[None] * displace
    return (lax.optimization_barrier(jnp.sum(weighted, 3)), -lax.optimization_barrier(jnp.sum(weighted, 2)), jnp.sum(energy), jnp.sum(slope * dist_sq))

def reference(positions, type_ids, counts, type_charge, type_sigma, type_epsilon):
    features = atom_table(positions, type_ids, counts, type_charge, type_sigma, type_epsilon)
    forces = jnp.zeros((3, NX, NY, NZ, ATOMS_CELL), jnp.float32)
    energy = jnp.float32(0.0)
    virial = jnp.float32(0.0)

    def rows_of(which):
        shift_x, shift_y, shift_z = corner_of(which)
        shifted = jnp.roll(features, (-shift_x, -shift_y, -shift_z), (1, 2, 3))
        return jnp.transpose(shifted, (1, 2, 0, 3, 4)).reshape((NX * NY, 7, NZ, ATOMS_CELL))

    def placed(force_rows, which):
        shift_x, shift_y, shift_z = corner_of(which)
        grid = jnp.transpose(force_rows.reshape((NX, NY, 3, NZ, ATOMS_CELL)), (2, 0, 1, 3, 4))
        return jnp.roll(grid, (shift_x, shift_y, shift_z), (1, 2, 3))
    for first_corner, second_corner in corner_pairs:
        offset = jnp.array([float(a - b) for a, b in zip(corner_of(second_corner), corner_of(first_corner))], jnp.float32)
        selfpair = first_corner == second_corner

        def one_row(member, offset=offset, selfpair=selfpair):
            return pair_terms(member[0], member[1], offset, selfpair)
        force_first, force_second, energies, virials = lax.map(one_row, (rows_of(first_corner), rows_of(second_corner)))
        forces = forces + placed(force_first, first_corner) + placed(force_second, second_corner)
        energy = energy + jnp.sum(energies)
        virial = virial + jnp.sum(virials)
    normaliser = 1.0 / (NX * NY * NZ * ATOMS_CELL)
    return (forces, jnp.stack([energy, virial]) * normaliser)
```

```python
import functools

import jax
import jax.numpy as jnp
from jax import lax
from jax.experimental import pallas as pl
from jax.experimental.pallas import tpu as pltpu
from jax.sharding import Mesh
from jax.sharding import PartitionSpec as P

GY = ("gy_0", "gy_1")
GZ = ("gz_0", "gz_1")
GX_GY_GZ = ("gx", "gy_0", "gy_1", "gz_0", "gz_1")

soft_core = 0.09
cut_sq = 1.0 + soft_core
far_away = 2.0
corner_pairs = [
    (first_corner, second_corner)
    for first_corner in range(8)
    for second_corner in range(8)
    if first_corner & second_corner == 0 and first_corner <= second_corner
]


def corner_of(which):
    return (which & 1, which >> 1 & 1, which >> 2 & 1)


def passed_along(value, axis, steps):
    count = lax.axis_size(axis)
    pairs = [(source, (source + steps) % count) for source in range(count)]
    return lax.ppermute(value, axis, pairs)


def one_axis_at_a_time(value, axes):
    return functools.reduce(lax.psum, axes, value)


def fill_tables(param_ref, table_ref):
    tile = (8, 128)
    charge = [jnp.full(tile, param_ref[0, kind], jnp.float32) for kind in range(2)]
    sigma = [jnp.full(tile, param_ref[1, kind], jnp.float32) for kind in range(2)]
    root = [jnp.sqrt(jnp.full(tile, param_ref[2, kind], jnp.float32)) for kind in range(2)]
    for first in range(2):
        for second in range(2):
            width = 0.5 * (sigma[first] + sigma[second])
            width_six = (width * width) * (width * width) * (width * width)
            attract = 24.0 * (root[first] * root[second]) * width_six
            repel = attract * width_six
            coulomb = charge[first] * charge[second]
            parts, inverse, square = pair_parts(jnp.full(tile, cut_sq, jnp.float32), attract, repel, coulomb)
            lennard, charged, steep = parts
            value = lennard * (1.0 / 6.0) + charged
            level = -(value + (square * inverse) * steep)
            for at, entry in enumerate((attract, repel, coulomb, steep, level)):
                table_ref[(first * 2 + second) * 5 + at] = entry


def pair_parts(square, attract, repel, coulomb):
    inverse = lax.rsqrt(square)
    two = inverse * inverse
    six = (two * two) * two
    pulled = attract * six
    pushed = repel * (six * six)
    lennard = pushed - pulled
    charged = coulomb * inverse
    steep = ((lennard + pushed) + charged) * inverse
    return (lennard, charged, steep), inverse, square


def fill_cell(cell_ref, column_ref, row_ref, kind_ref, cell, place, as_first):
    atoms = cell_ref[cell]
    row = lax.broadcasted_iota(jnp.int32, (8, 128), 0)
    shift = jnp.where(row == 0, place[0], jnp.where(row == 1, place[1], place[2]))
    spot = jnp.where(row < 3, atoms + shift, 0.0)
    norm = jnp.sum(spot * spot, 0, keepdims=True) + 0.5 * soft_core + far_away * (1.0 - atoms[4:5])
    whole = jnp.where(row == 3, jnp.broadcast_to(norm, (8, 128)), spot)
    high = whole.astype(jnp.bfloat16).astype(jnp.float32)
    middle = (whole - high).astype(jnp.bfloat16).astype(jnp.float32)
    low = ((whole - high) - middle).astype(jnp.bfloat16).astype(jnp.float32)

    def down(value, by):
        return pltpu.roll(value, by, 0)

    xyz = row < 3
    xyz_down = (row > 3) & (row < 7)
    middle_down = jnp.where(xyz_down, down(middle, 4), 0.0)
    rows = [
        jnp.where(xyz, high, jnp.where(xyz_down, middle_down, 1.0)),
        jnp.where(
            xyz,
            low,
            jnp.where(
                row == 3,
                1.0,
                jnp.where(
                    row == 4,
                    down(high, 1),
                    jnp.where(row == 5, down(middle, 2), jnp.where(row == 6, down(low, 3), 0.0)),
                ),
            ),
        ),
        jnp.where(xyz, high, middle_down),
        jnp.where(xyz, high, 0.0),
    ]
    row_ref[cell] = jnp.concatenate(rows, 0).astype(jnp.bfloat16)
    if not as_first:
        return
    high_two = -2.0 * high
    middle_two = -2.0 * middle
    columns = [
        jnp.where(
            row < 4,
            jnp.where(xyz, high_two, high),
            down(jnp.where(xyz, high_two, middle), 4),
        ),
        jnp.where(xyz, high_two, jnp.where(row == 3, low, jnp.where(row == 7, 0.0, 1.0))),
        jnp.where(xyz, middle_two, jnp.where(xyz_down, down(middle_two, 4), 0.0)),
        jnp.where(xyz, -2.0 * low, 0.0),
    ]
    stacked = jnp.concatenate(columns + [jnp.zeros((96, 128), jnp.float32)], 0)
    column_ref[cell] = jnp.transpose(stacked)[:, :32].astype(jnp.bfloat16)
    kind_ref[cell] = jnp.transpose(jnp.broadcast_to(atoms[3:4], (128, 128)))


def pair_kernel(sizes, param_ref, cell_ref, force_ref, total_ref, column_ref, row_ref, kind_ref, table_ref, sum_ref):
    size_x, size_y, size_z = sizes
    wide_y, wide_z = size_y + 1, size_z + 1
    cells = (size_x + 1) * wide_y * wide_z
    fill_tables(param_ref, table_ref)

    def middle_of(cell):
        at = (cell // (wide_y * wide_z), cell // wide_z % wide_y, cell % wide_z)
        return [float(a) - (size + 1) / 2 for a, size in zip(at, sizes)]

    for cell in range(cells):
        fill_cell(cell_ref, column_ref, row_ref, kind_ref, cell, middle_of(cell), cell % wide_z < size_z)
    sum_ref[...] = jnp.zeros_like(sum_ref)
    tile = (8, 128)

    def block(first, second, selfpair, energy):
        square = lax.dot_general(
            column_ref[first], row_ref[second], (((1,), (0,)), ((), ())), preferred_element_type=jnp.float32
        )
        kind_second = jnp.broadcast_to(cell_ref[second, 3:4], tile) > 0.5
        rows = [
            [
                jnp.where(kind_second, table_ref[(kind * 2 + 1) * 5 + at], table_ref[kind * 2 * 5 + at])
                for at in range(5)
            ]
            for kind in range(2)
        ]
        highs, lows = [], []
        partial = jnp.zeros(tile, jnp.float32)
        for pack in range(8):
            slopes = []
            for half in range(2):
                at = pack * 16 + half * 8
                kind_first = kind_ref[first, at : at + 8, :] > 0.5
                attract, repel, coulomb, steep_cut, level = (
                    jnp.where(kind_first, one, zero) for zero, one in zip(*rows)
                )
                here = square[at : at + 8]
                if selfpair:
                    lane = lax.broadcasted_iota(jnp.int32, tile, 1)
                    sublane = lax.broadcasted_iota(jnp.int32, tile, 0)
                    here = jnp.where(lane == sublane + at, cut_sq, here)
                (lennard, charged, steep), inverse, here = pair_parts(
                    jnp.minimum(here, cut_sq), attract, repel, coulomb
                )
                value = lennard * (1.0 / 6.0) + charged
                partial = partial + ((value + (here * inverse) * steep_cut) + level)
                slopes.append((steep - steep_cut) * inverse)
            slope = jnp.concatenate(slopes, 0)
            high = slope.astype(jnp.bfloat16)
            highs.append(high)
            lows.append((slope - high.astype(jnp.float32)).astype(jnp.bfloat16))
        high = jnp.concatenate(highs, 0)
        low = jnp.concatenate(lows, 0)
        across = (((1,), (1,)), ((), ()))
        along = (((1,), (0,)), ((), ()))
        dot = functools.partial(lax.dot_general, preferred_element_type=jnp.float32)
        of_second = row_ref[second, 0:16, :]
        on_first = dot(of_second, high, across) + dot(of_second, low, across)
        if selfpair:
            return on_first, None, energy + 0.5 * partial
        of_first = row_ref[first, 0:16, :]
        on_second = dot(of_first, high, along) + dot(of_first, low, along)
        return on_first, on_second, energy + partial

    def one_cell(member, energy):
        base = (
            member // (size_y * size_z) * (wide_y * wide_z)
            + member // size_z % size_y * wide_z
            + member % size_z
        )
        for first_corner, second_corner in corner_pairs:
            first, second = (
                base + x * (wide_y * wide_z) + y * wide_z + z
                for x, y, z in (corner_of(first_corner), corner_of(second_corner))
            )
            on_first, on_second, energy = block(first, second, first_corner == second_corner, energy)
            sum_ref[first] = sum_ref[first] + on_first
            if on_second is not None:
                sum_ref[second] = sum_ref[second] + on_second
        return energy

    energy = lax.fori_loop(0, size_x * size_y * size_z, one_cell, jnp.zeros(tile, jnp.float32))
    total_ref[0] = energy
    virial = jnp.zeros((1, 128), jnp.float32)
    row = lax.broadcasted_iota(jnp.int32, tile, 0)
    for cell in range(cells):
        place = middle_of(cell)
        shift = jnp.where(row == 0, place[0], jnp.where(row == 1, place[1], place[2]))
        spot = jnp.where(row < 3, cell_ref[cell] + shift, 0.0)
        upper, lower = sum_ref[cell, 0:8, :], sum_ref[cell, 8:16, :]
        moved = jnp.where(row < 3, upper + pltpu.roll(upper, 4, 0) + lower, 0.0)
        slopes = upper[3:4]
        norm = (
            jnp.sum(spot * spot, 0, keepdims=True)
            + (0.5 * soft_core - soft_core)
            + far_away * (1.0 - cell_ref[cell, 4:5])
        )
        crossed = lower[4:5] + lower[5:6] + lower[6:7]
        virial = virial + (norm * slopes + crossed - 2.0 * jnp.sum(spot * moved, 0, keepdims=True))
        force_ref[cell] = spot * slopes - moved
    total_ref[1] = jnp.where(row == 0, jnp.broadcast_to(-0.5 * virial, tile), 0.0)


def pair_sums(params, atoms, sizes):
    cells = atoms.shape[0]
    return pl.pallas_call(
        functools.partial(pair_kernel, sizes),
        out_shape=(
            jax.ShapeDtypeStruct((cells, 8, 128), jnp.float32),
            jax.ShapeDtypeStruct((2, 8, 128), jnp.float32),
        ),
        in_specs=[
            pl.BlockSpec(memory_space=pltpu.SMEM),
            pl.BlockSpec(memory_space=pltpu.VMEM),
        ],
        out_specs=(
            pl.BlockSpec(memory_space=pltpu.VMEM),
            pl.BlockSpec(memory_space=pltpu.VMEM),
        ),
        scratch_shapes=[
            pltpu.VMEM((cells, 128, 32), jnp.bfloat16),
            pltpu.VMEM((cells, 32, 128), jnp.bfloat16),
            pltpu.VMEM((cells, 128, 128), jnp.float32),
            pltpu.VMEM((20, 8, 128), jnp.float32),
            pltpu.VMEM((cells, 16, 128), jnp.float32),
        ],
        name="pair_sums",
    )(params, atoms)


def per_device(positions, type_ids, counts, type_charge, type_sigma, type_epsilon):
    size_x, size_y, size_z, width_atoms = positions.shape[1:]
    slots = lax.broadcasted_iota(jnp.int32, type_ids.shape, 3)
    occupied = (slots < counts[..., None]).astype(jnp.float32)
    blank = jnp.zeros(type_ids.shape, jnp.float32)
    atoms = jnp.stack(
        [positions[0], positions[1], positions[2], type_ids.astype(jnp.float32), occupied, blank, blank, blank], 3
    )
    extended = jnp.concatenate([atoms, passed_along(atoms[:1], "gx", -1)], 0)
    extended = jnp.concatenate([extended, passed_along(extended[:, :1], GY, -1)], 1)
    extended = jnp.concatenate([extended, passed_along(extended[:, :, :1], GZ, -1)], 2)
    wide = extended.shape[:3]
    params = jnp.stack([type_charge, type_sigma, type_epsilon])
    forces, sums = pair_sums(
        params, extended.reshape((-1, 8, width_atoms)), (size_x, size_y, size_z)
    )
    reaction = forces.reshape(wide + (8, width_atoms))[..., :3, :]
    returned = passed_along(reaction[:, :, size_z:], GZ, 1)
    reaction = reaction[:, :, :size_z].at[:, :, :1].add(returned)
    returned = passed_along(reaction[:, size_y:], GY, 1)
    reaction = reaction[:, :size_y].at[:, :1].add(returned)
    returned = passed_along(reaction[size_x:], "gx", 1)
    forces = reaction[:size_x].at[:1].add(returned)
    summed = one_axis_at_a_time(jnp.sum(sums, (1, 2)), GX_GY_GZ)
    normaliser = 1.0 / (
        size_x
        * lax.axis_size("gx")
        * size_y
        * lax.axis_size(GY)
        * size_z
        * lax.axis_size(GZ)
        * width_atoms
    )
    return (jnp.transpose(forces, (3, 0, 1, 2, 4)), summed * normaliser)


def solution(mesh):
    split = Mesh(
        mesh.devices.reshape(mesh.shape["gx"], 4, 2, 3, 4), ("gx", "gy_0", "gy_1", "gz_0", "gz_1")
    )
    placed = (P(None, "gx", GY, GZ, None), P("gx", GY, GZ, None), P("gx", GY, GZ), P(), P(), P())
    return jax.shard_map(
        per_device,
        mesh=split,
        in_specs=placed,
        out_specs=(P(None, "gx", GY, GZ, None), P()),
        check_vma=False,
    )
```

```python
import functools

import jax
import jax.numpy as jnp
from jax import lax
from jax.experimental import pallas as pl
from jax.experimental.pallas import tpu as pltpu
from jax.sharding import Mesh
from jax.sharding import PartitionSpec as P

GY = ("gy_0", "gy_1")
GZ = ("gz_0", "gz_1")
GX_GY = ("gx", "gy_0", "gy_1")

soft_core = 0.09
cut_sq = 1.0 + soft_core
far_away = 2.0
AHEAD = 2
BEHIND = 1
corner_pairs = [
    (first_corner, second_corner)
    for first_corner in range(8)
    for second_corner in range(8)
    if first_corner & second_corner == 0 and first_corner <= second_corner
]


def corner_of(which):
    return (which & 1, which >> 1 & 1, which >> 2 & 1)


def passed_along(value, axis, steps):
    count = lax.axis_size(axis)
    pairs = [(source, (source + steps) % count) for source in range(count)]
    return lax.ppermute(value, axis, pairs)


def fill_tables(param_ref, table_ref):
    tile = (8, 128)
    charge = [jnp.full(tile, param_ref[0, kind], jnp.float32) for kind in range(2)]
    sigma = [jnp.full(tile, param_ref[1, kind], jnp.float32) for kind in range(2)]
    root = [jnp.sqrt(jnp.full(tile, param_ref[2, kind], jnp.float32)) for kind in range(2)]
    for first in range(2):
        for second in range(2):
            width = 0.5 * (sigma[first] + sigma[second])
            width_six = (width * width) * (width * width) * (width * width)
            attract = 24.0 * (root[first] * root[second]) * width_six
            repel = attract * width_six
            coulomb = charge[first] * charge[second]
            parts, inverse, square = pair_parts(jnp.full(tile, cut_sq, jnp.float32), attract, repel, coulomb)
            lennard, charged, steep = parts
            value = lennard * (1.0 / 6.0) + charged
            level = -(value + (square * inverse) * steep)
            for at, entry in enumerate((attract, repel, coulomb, steep, level)):
                table_ref[(first * 2 + second) * 5 + at] = entry


def pair_parts(square, attract, repel, coulomb):
    inverse = lax.rsqrt(square)
    two = inverse * inverse
    six = (two * two) * two
    pulled = attract * six
    pushed = repel * (six * six)
    lennard = pushed - pulled
    charged = coulomb * inverse
    steep = ((lennard + pushed) + charged) * inverse
    return (lennard, charged, steep), inverse, square


def fill_cell(cell_ref, column_ref, row_ref, kind_ref, cell, place, as_first):
    atoms = cell_ref[cell]
    row = lax.broadcasted_iota(jnp.int32, (8, 128), 0)
    shift = jnp.where(row == 0, place[0], jnp.where(row == 1, place[1], place[2]))
    spot = jnp.where(row < 3, atoms + shift, 0.0)
    norm = jnp.sum(spot * spot, 0, keepdims=True) + 0.5 * soft_core + far_away * (1.0 - atoms[4:5])
    whole = jnp.where(row == 3, jnp.broadcast_to(norm, (8, 128)), spot)
    high = whole.astype(jnp.bfloat16).astype(jnp.float32)
    middle = (whole - high).astype(jnp.bfloat16).astype(jnp.float32)
    low = ((whole - high) - middle).astype(jnp.bfloat16).astype(jnp.float32)

    def down(value, by):
        return pltpu.roll(value, by, 0)

    xyz = row < 3
    xyz_down = (row > 3) & (row < 7)
    middle_down = jnp.where(xyz_down, down(middle, 4), 0.0)
    rows = [
        jnp.where(xyz, high, jnp.where(xyz_down, middle_down, 1.0)),
        jnp.where(
            xyz,
            low,
            jnp.where(
                row == 3,
                1.0,
                jnp.where(
                    row == 4,
                    down(high, 1),
                    jnp.where(row == 5, down(middle, 2), jnp.where(row == 6, down(low, 3), 0.0)),
                ),
            ),
        ),
        jnp.where(xyz, high, middle_down),
        jnp.where(xyz, high, 0.0),
    ]
    row_ref[cell] = jnp.concatenate(rows, 0).astype(jnp.bfloat16)
    if not as_first:
        return
    high_two = -2.0 * high
    middle_two = -2.0 * middle
    columns = [
        jnp.where(
            row < 4,
            jnp.where(xyz, high_two, high),
            down(jnp.where(xyz, high_two, middle), 4),
        ),
        jnp.where(xyz, high_two, jnp.where(row == 3, low, jnp.where(row == 7, 0.0, 1.0))),
        jnp.where(xyz, middle_two, jnp.where(xyz_down, down(middle_two, 4), 0.0)),
        jnp.where(xyz, -2.0 * low, 0.0),
    ]
    stacked = jnp.concatenate(columns + [jnp.zeros((96, 128), jnp.float32)], 0)
    column_ref[cell] = jnp.transpose(stacked)[:, :32].astype(jnp.bfloat16)
    kind_ref[cell] = jnp.transpose(jnp.broadcast_to(atoms[3:4], (128, 128)))


def pair_kernel(sizes, param_ref, cell_ref, force_ref, total_ref, column_ref, row_ref, kind_ref, table_ref, sum_ref, square_ref, high_ref, low_ref):
    size_x, size_y, size_z = sizes
    wide_y, wide_z = size_y + 1, size_z + 1
    cells = (size_x + 1) * wide_y * wide_z
    fill_tables(param_ref, table_ref)

    def middle_of(cell):
        at = (cell // (wide_y * wide_z), cell // wide_z % wide_y, cell % wide_z)
        return [float(a) - (size + 1) / 2 for a, size in zip(at, sizes)]

    for cell in range(cells):
        fill_cell(cell_ref, column_ref, row_ref, kind_ref, cell, middle_of(cell), cell % wide_z < size_z)
    sum_ref[...] = jnp.zeros_like(sum_ref)
    tile = (8, 128)

    across = (((1,), (1,)), ((), ()))
    along = (((1,), (0,)), ((), ()))
    dot = functools.partial(lax.dot_general, preferred_element_type=jnp.float32)

    def apart(at_pair, first, second):
        square_ref[at_pair] = dot(column_ref[first], row_ref[second], along)

    def slopes_of(at_pair, first, second, selfpair):
        kind_second = jnp.broadcast_to(cell_ref[second, 3:4], tile) > 0.5
        rows = [
            [
                jnp.where(kind_second, table_ref[(kind * 2 + 1) * 5 + at], table_ref[kind * 2 * 5 + at])
                for at in range(5)
            ]
            for kind in range(2)
        ]
        partial = jnp.zeros(tile, jnp.float32)
        for pack in range(8):
            slopes = []
            for half in range(2):
                at = pack * 16 + half * 8
                kind_first = kind_ref[first, at : at + 8, :] > 0.5
                attract, repel, coulomb, steep_cut, level = (
                    jnp.where(kind_first, one, zero) for zero, one in zip(*rows)
                )
                here = square_ref[at_pair, at : at + 8]
                if selfpair:
                    lane = lax.broadcasted_iota(jnp.int32, tile, 1)
                    sublane = lax.broadcasted_iota(jnp.int32, tile, 0)
                    here = jnp.where(lane == sublane + at, cut_sq, here)
                (lennard, charged, steep), inverse, here = pair_parts(
                    jnp.minimum(here, cut_sq), attract, repel, coulomb
                )
                value = lennard * (1.0 / 6.0) + charged
                partial = partial + ((value + (here * inverse) * steep_cut) + level)
                slopes.append((steep - steep_cut) * inverse)
            slope = jnp.concatenate(slopes, 0)
            high = slope.astype(jnp.bfloat16)
            high_ref[at_pair, pack * 16 : pack * 16 + 16] = high
            low_ref[at_pair, pack * 16 : pack * 16 + 16] = (slope - high.astype(jnp.float32)).astype(jnp.bfloat16)
        return 0.5 * partial if selfpair else partial

    def push(at_pair, first, second, selfpair):
        high, low = high_ref[at_pair], low_ref[at_pair]
        of_second = row_ref[second, 0:16, :]
        on_first = dot(of_second, high, across) + dot(of_second, low, across)
        sum_ref[first] = sum_ref[first] + on_first
        if selfpair:
            return
        of_first = row_ref[first, 0:16, :]
        on_second = dot(of_first, high, along) + dot(of_first, low, along)
        sum_ref[second] = sum_ref[second] + on_second

    def one_cell(member, energy):
        base = (
            member // (size_y * size_z) * (wide_y * wide_z)
            + member // size_z % size_y * wide_z
            + member % size_z
        )
        pairs = []
        for first_corner, second_corner in corner_pairs:
            first, second = (
                base + x * (wide_y * wide_z) + y * wide_z + z
                for x, y, z in (corner_of(first_corner), corner_of(second_corner))
            )
            pairs.append((len(pairs), first, second, first_corner == second_corner))
        for step in range(len(pairs) + AHEAD + BEHIND):
            if step < len(pairs):
                apart(*pairs[step][:3])
            if 0 <= step - AHEAD < len(pairs):
                energy = energy + slopes_of(*pairs[step - AHEAD])
            if step >= AHEAD + BEHIND:
                push(*pairs[step - AHEAD - BEHIND])
        return energy

    energy = lax.fori_loop(0, size_x * size_y * size_z, one_cell, jnp.zeros(tile, jnp.float32))
    virial = jnp.zeros((1, 128), jnp.float32)
    row = lax.broadcasted_iota(jnp.int32, tile, 0)
    for cell in range(cells):
        place = middle_of(cell)
        shift = jnp.where(row == 0, place[0], jnp.where(row == 1, place[1], place[2]))
        spot = jnp.where(row < 3, cell_ref[cell] + shift, 0.0)
        upper, lower = sum_ref[cell, 0:8, :], sum_ref[cell, 8:16, :]
        moved = jnp.where(row < 3, upper + pltpu.roll(upper, 4, 0) + lower, 0.0)
        slopes = upper[3:4]
        norm = (
            jnp.sum(spot * spot, 0, keepdims=True)
            + (0.5 * soft_core - soft_core)
            + far_away * (1.0 - cell_ref[cell, 4:5])
        )
        crossed = lower[4:5] + lower[5:6] + lower[6:7]
        virial = virial + (norm * slopes + crossed - 2.0 * jnp.sum(spot * moved, 0, keepdims=True))
        force_ref[cell] = spot * slopes - moved
    lane = lax.broadcasted_iota(jnp.int32, total_ref.shape, 1)
    total_ref[...] = jnp.where(lane == 0, jnp.sum(energy), jnp.where(lane == 1, -0.5 * jnp.sum(virial), 0.0))


def pair_sums(params, atoms, sizes, copies):
    cells = atoms.shape[0]
    return pl.pallas_call(
        functools.partial(pair_kernel, sizes),
        out_shape=(
            jax.ShapeDtypeStruct((cells, 8, 128), jnp.float32),
            jax.ShapeDtypeStruct((copies, 128), jnp.float32),
        ),
        in_specs=[
            pl.BlockSpec(memory_space=pltpu.SMEM),
            pl.BlockSpec(memory_space=pltpu.VMEM),
        ],
        out_specs=(
            pl.BlockSpec(memory_space=pltpu.VMEM),
            pl.BlockSpec(memory_space=pltpu.VMEM),
        ),
        scratch_shapes=[
            pltpu.VMEM((cells, 128, 32), jnp.bfloat16),
            pltpu.VMEM((cells, 32, 128), jnp.bfloat16),
            pltpu.VMEM((cells, 128, 128), jnp.float32),
            pltpu.VMEM((20, 8, 128), jnp.float32),
            pltpu.VMEM((cells, 16, 128), jnp.float32),
            pltpu.VMEM((len(corner_pairs), 128, 128), jnp.float32),
            pltpu.VMEM((len(corner_pairs), 128, 128), jnp.bfloat16),
            pltpu.VMEM((len(corner_pairs), 128, 128), jnp.bfloat16),
        ],
        name="pair_sums",
    )(params, atoms)


def per_device(positions, type_ids, counts, type_charge, type_sigma, type_epsilon):
    size_x, size_y, size_z, width_atoms = positions.shape[1:]
    slots = lax.broadcasted_iota(jnp.int32, type_ids.shape, 3)
    occupied = (slots < counts[..., None]).astype(jnp.float32)
    blank = jnp.zeros(type_ids.shape, jnp.float32)
    atoms = jnp.stack(
        [positions[0], positions[1], positions[2], type_ids.astype(jnp.float32), occupied, blank, blank, blank], 3
    )
    extended = jnp.concatenate([atoms, passed_along(atoms[:1], "gx", -1)], 0)
    extended = jnp.concatenate([extended, passed_along(extended[:, :1], GY, -1)], 1)
    extended = jnp.concatenate([extended, passed_along(extended[:, :, :1], GZ, -1)], 2)
    wide = extended.shape[:3]
    params = jnp.stack([type_charge, type_sigma, type_epsilon])
    forces, sums = pair_sums(
        params,
        extended.reshape((-1, 8, width_atoms)),
        (size_x, size_y, size_z),
        lax.axis_size(GX_GY),
    )
    reaction = forces.reshape(wide + (8, width_atoms))[..., :3, :]
    returned = passed_along(reaction[:, :, size_z:], GZ, 1)
    reaction = reaction[:, :, :size_z].at[:, :, :1].add(returned)
    returned = passed_along(reaction[:, size_y:], GY, 1)
    reaction = reaction[:, :size_y].at[:, :1].add(returned)
    returned = passed_along(reaction[size_x:], "gx", 1)
    forces = reaction[:size_x].at[:1].add(returned)
    rows = jnp.sum(lax.all_to_all(sums, GX_GY, 0, 0, tiled=True), 0)
    copies = jnp.broadcast_to(rows, (lax.axis_size(GZ), width_atoms))
    summed = jnp.sum(lax.all_to_all(copies, GZ, 0, 0, tiled=True), 0)[:2]
    normaliser = 1.0 / (
        size_x
        * lax.axis_size("gx")
        * size_y
        * lax.axis_size(GY)
        * size_z
        * lax.axis_size(GZ)
        * width_atoms
    )
    return (jnp.transpose(forces, (3, 0, 1, 2, 4)), summed * normaliser)


def solution(mesh):
    split = Mesh(
        mesh.devices.reshape(mesh.shape["gx"], 4, 2, 3, 4), ("gx", "gy_0", "gy_1", "gz_0", "gz_1")
    )
    placed = (P(None, "gx", GY, GZ, None), P("gx", GY, GZ, None), P("gx", GY, GZ), P(), P(), P())
    return jax.shard_map(
        per_device,
        mesh=split,
        in_specs=placed,
        out_specs=(P(None, "gx", GY, GZ, None), P()),
        check_vma=False,
    )
```

```python
import dataclasses
import functools
import itertools

import jax
import jax.numpy as jnp
from jax import lax
from jax.experimental import pallas as pl
from jax.experimental.pallas import tpu as pltpu
from jax.sharding import Mesh
from jax.sharding import PartitionSpec as P

GY = ("gy_0", "gy_1")
GZ = ("gz_0", "gz_1")
ONE = ("gx", "gz_1")
OTHER = ("gy_0", "gy_1", "gz_0")

soft_core = 0.09
cut_sq = 1.0 + soft_core
far_away = 2.0
GROUP = 12
corner_pairs = [
    (first_corner, second_corner)
    for first_corner in range(8)
    for second_corner in range(8)
    if first_corner & second_corner == 0 and first_corner <= second_corner
]


def corner_of(which):
    return (which & 1, which >> 1 & 1, which >> 2 & 1)


def passed_along(value, axis, steps):
    count = lax.axis_size(axis)
    pairs = [(source, (source + steps) % count) for source in range(count)]
    return lax.ppermute(value, axis, pairs)


def fill_tables(param_ref, coef_ref):
    tile = (8, 128)
    charge = [jnp.full(tile, param_ref[0, kind], jnp.float32) for kind in range(2)]
    sigma = [jnp.full(tile, param_ref[1, kind], jnp.float32) for kind in range(2)]
    root = [jnp.sqrt(jnp.full(tile, param_ref[2, kind], jnp.float32)) for kind in range(2)]
    for first in range(2):
        for second in range(2):
            width = 0.5 * (sigma[first] + sigma[second])
            width_six = (width * width) * (width * width) * (width * width)
            attract = 24.0 * (root[first] * root[second]) * width_six
            repel = attract * width_six
            coulomb = charge[first] * charge[second]
            value, steep, _ = pair_parts(jnp.full(tile, cut_sq, jnp.float32), attract, repel, coulomb)
            level = -value
            for at, entry in enumerate((attract, repel, coulomb, steep, level)):
                coef_ref[(first * 2 + second) * 5 + at] = entry


def pair_parts(square, attract, repel, coulomb):
    inverse = lax.rsqrt(square)
    two = inverse * inverse
    six = (two * two) * two
    pulled = attract * six
    pushed = repel * (six * six)
    lennard = pushed - pulled
    charged = coulomb * inverse
    moment = (lennard + pushed) + charged
    return (lennard * (1.0 / 6.0) + charged) + moment, moment * inverse, inverse


def fill_cell(cell_ref, column_ref, row_ref, kind_ref, cell, place, as_first):
    atoms = cell_ref[cell]
    row = lax.broadcasted_iota(jnp.int32, (8, 128), 0)
    shift = jnp.where(row == 0, place[0], jnp.where(row == 1, place[1], place[2]))
    spot = jnp.where(row < 3, atoms + shift, 0.0)
    norm = jnp.sum(spot * spot, 0, keepdims=True) + 0.5 * soft_core + far_away * (1.0 - atoms[4:5])
    whole = jnp.where(row == 3, jnp.broadcast_to(norm, (8, 128)), spot)
    high = whole.astype(jnp.bfloat16).astype(jnp.float32)
    middle = (whole - high).astype(jnp.bfloat16).astype(jnp.float32)
    low = ((whole - high) - middle).astype(jnp.bfloat16).astype(jnp.float32)

    def down(value, by):
        return pltpu.roll(value, by, 0)

    xyz = row < 3
    xyz_down = (row > 3) & (row < 7)
    middle_down = jnp.where(xyz_down, down(middle, 4), 0.0)
    rows = [
        jnp.where(xyz, high, jnp.where(xyz_down, middle_down, 1.0)),
        jnp.where(
            xyz,
            low,
            jnp.where(
                row == 3,
                1.0,
                jnp.where(
                    row == 4,
                    down(high, 1),
                    jnp.where(row == 5, down(middle, 2), jnp.where(row == 6, down(low, 3), 0.0)),
                ),
            ),
        ),
        jnp.where(xyz, high, middle_down),
        jnp.where(xyz, high, 0.0),
    ]
    row_ref[cell] = jnp.concatenate(rows, 0).astype(jnp.bfloat16)
    if not as_first:
        return
    high_two = -2.0 * high
    middle_two = -2.0 * middle
    columns = [
        jnp.where(
            row < 4,
            jnp.where(xyz, high_two, high),
            down(jnp.where(xyz, high_two, middle), 4),
        ),
        jnp.where(xyz, high_two, jnp.where(row == 3, low, jnp.where(row == 7, 0.0, 1.0))),
        jnp.where(xyz, middle_two, jnp.where(xyz_down, down(middle_two, 4), 0.0)),
        jnp.where(xyz, -2.0 * low, 0.0),
    ]
    columns[3] = jnp.where(row == 7, jnp.broadcast_to(atoms[3:4], (8, 128)), columns[3])
    turned = jnp.transpose(jnp.concatenate(columns, 0))
    column_ref[cell] = turned.astype(jnp.bfloat16)
    kind_ref[cell] = jnp.broadcast_to(turned[:, 31:32], (128, 128))


def pair_kernel(plan, *refs):
    refs = list(refs)
    param_ref, table_ref, cell_ref = refs[:3]
    refs = refs[3:]
    before_ref = refs.pop(0) if plan.added else None
    force_ref, total_ref, sum_ref, column_ref, row_ref, kind_ref, coef_ref, square_ref, high_ref, low_ref = refs
    cells = len(plan.places)
    tile = (8, 128)
    fill_tables(param_ref, coef_ref)
    for cell in range(cells):
        fill_cell(cell_ref, column_ref, row_ref, kind_ref, cell, plan.places[cell], plan.firsts[cell])
    sum_ref[...] = jnp.zeros_like(sum_ref)
    energy = jnp.zeros(tile, jnp.float32)

    across = (((1,), (1,)), ((), ()))
    along = (((1,), (0,)), ((), ()))
    dot = functools.partial(lax.dot_general, preferred_element_type=jnp.float32)

    def apart(slot, first, second):
        square_ref[slot] = dot(column_ref[first], row_ref[second], along)

    def slopes_of(slot, first, second, selfpair):
        kind_second = jnp.broadcast_to(cell_ref[second, 3:4], tile) > 0.5
        rows = [
            [
                jnp.where(kind_second, coef_ref[(kind * 2 + 1) * 5 + at], coef_ref[kind * 2 * 5 + at])
                for at in range(5)
            ]
            for kind in range(2)
        ]
        partial = jnp.zeros(tile, jnp.float32)
        for pack in range(8):
            slopes = []
            for half in range(2):
                at = pack * 16 + half * 8
                kind_first = kind_ref[first, at : at + 8, :] > 0.5
                attract, repel, coulomb, steep_cut, level = (
                    jnp.where(kind_first, one, zero) for zero, one in zip(*rows)
                )
                here = square_ref[slot, at : at + 8]
                if selfpair:
                    lane = lax.broadcasted_iota(jnp.int32, tile, 1)
                    sublane = lax.broadcasted_iota(jnp.int32, tile, 0)
                    here = jnp.where(lane == sublane + at, cut_sq, here)
                value, steep, inverse = pair_parts(jnp.minimum(here, cut_sq), attract, repel, coulomb)
                partial = partial + (value + level)
                slopes.append((steep - steep_cut) * inverse)
            slope = jnp.concatenate(slopes, 0)
            high = slope.astype(jnp.bfloat16)
            high_ref[slot, pack * 16 : pack * 16 + 16] = high
            low_ref[slot, pack * 16 : pack * 16 + 16] = (slope - high.astype(jnp.float32)).astype(jnp.bfloat16)
        return 0.5 * partial if selfpair else partial

    def push(slot, first, second, selfpair):
        high, low = high_ref[slot], low_ref[slot]
        of_second = row_ref[second, 0:16, :]
        on_first = dot(of_second, high, across) + dot(of_second, low, across)
        sum_ref[first] = sum_ref[first] + on_first
        if selfpair:
            return
        of_first = row_ref[first, 0:16, :]
        on_second = dot(of_first, high, along) + dot(of_first, low, along)
        sum_ref[second] = sum_ref[second] + on_second

    def run(start, rounds, group, selfpair, energy):
        if not rounds:
            return energy

        def cells_of(at):
            return table_ref[2 * at], table_ref[2 * at + 1]

        for slot in range(group):
            apart(slot, *cells_of(start + slot))
        high_ref[group - 1] = jnp.zeros((128, 128), jnp.bfloat16)
        low_ref[group - 1] = jnp.zeros((128, 128), jnp.bfloat16)

        def one_round(index, energy):
            base = start + index * group
            following = start + jnp.minimum(index + 1, rounds - 1) * group
            for slot in range(group):
                energy = energy + slopes_of(slot, *cells_of(base + slot), selfpair)
                apart(slot, *cells_of(following + slot))
                if slot:
                    push(slot - 1, *cells_of(base + slot - 1), selfpair)
                else:
                    push(group - 1, *cells_of(jnp.maximum(base - 1, start)), selfpair)
            return energy

        energy = lax.fori_loop(0, rounds, one_round, energy)
        push(group - 1, *cells_of(start + rounds * group - 1), selfpair)
        return energy

    start = 0
    for rounds, group, selfpair in plan.runs:
        energy = run(start, rounds, group, selfpair, energy)
        start += rounds * group
    moment = jnp.zeros((1, 128), jnp.float32)
    steepness = jnp.zeros((1, 128), jnp.float32)
    row = lax.broadcasted_iota(jnp.int32, tile, 0)
    for cell in range(cells):
        place = plan.places[cell]
        shift = jnp.where(row == 0, place[0], jnp.where(row == 1, place[1], place[2]))
        spot = jnp.where(row < 3, cell_ref[cell] + shift, 0.0)
        upper, lower = sum_ref[cell, 0:8, :], sum_ref[cell, 8:16, :]
        moved = jnp.where(row < 3, upper + pltpu.roll(upper, 4, 0) + lower, 0.0)
        slopes = upper[3:4]
        norm = (
            jnp.sum(spot * spot, 0, keepdims=True)
            + 0.5 * soft_core
            + far_away * (1.0 - cell_ref[cell, 4:5])
        )
        crossed = lower[4:5] + lower[5:6] + lower[6:7]
        moment = moment + (norm * slopes + crossed - 2.0 * jnp.sum(spot * moved, 0, keepdims=True))
        steepness = steepness + slopes
        force_ref[cell] = spot * slopes - moved
    lane = lax.broadcasted_iota(jnp.int32, total_ref.shape, 1)
    virial = 0.5 * (soft_core * jnp.sum(steepness) - jnp.sum(moment))
    total = jnp.where(
        lane == 0, jnp.sum(energy) - 0.5 * jnp.sum(moment), jnp.where(lane == 1, virial, 0.0)
    )
    total_ref[...] = total + before_ref[0:1] if plan.added else total


@dataclasses.dataclass(frozen=True)
class Plan:
    places: tuple
    firsts: tuple
    runs: tuple
    added: bool
    copies: int


def rounds_of(pairs, group):
    if not pairs:
        return ()
    group = max(g for g in range(1, group + 1) if len(pairs) % g == 0)
    return ((len(pairs) // group, group, pairs[0][0] == pairs[0][1]),)


def pair_sums(plan, table, params, atoms, *before):
    cells = len(plan.places)
    vmem = pl.BlockSpec(memory_space=pltpu.VMEM)
    smem = pl.BlockSpec(memory_space=pltpu.SMEM)
    slots = max(group for _, group, _ in plan.runs)
    sums = (cells, 16, 128)
    shapes = [(cells, 8, 128), (plan.copies, 128)]
    return pl.pallas_call(
        functools.partial(pair_kernel, plan),
        out_shape=tuple(jax.ShapeDtypeStruct(shape, jnp.float32) for shape in shapes),
        in_specs=[smem, smem, vmem] + [vmem] * len(before),
        out_specs=(vmem, vmem),
        scratch_shapes=[
            pltpu.VMEM(sums, jnp.float32),
            pltpu.VMEM((cells, 128, 32), jnp.bfloat16),
            pltpu.VMEM((cells, 32, 128), jnp.bfloat16),
            pltpu.VMEM((cells, 128, 128), jnp.float32),
            pltpu.VMEM((20, 8, 128), jnp.float32),
            pltpu.VMEM((slots, 128, 128), jnp.float32),
            pltpu.VMEM((slots, 128, 128), jnp.bfloat16),
            pltpu.VMEM((slots, 128, 128), jnp.bfloat16),
        ],
        name="pair_sums",
    )(params, jnp.array(table, jnp.int32).reshape(-1), atoms, *before)


def pair_lists(sizes):
    alone, inside, beyond = [], [], []
    for member in itertools.product(*map(range, sizes)):
        for corners in corner_pairs:
            pair = tuple(tuple(m + c for m, c in zip(member, corner_of(which))) for which in corners)
            if pair[0] == pair[1]:
                alone.append(pair)
            elif all(at < size for cell in pair for at, size in zip(cell, sizes)):
                inside.append(pair)
            else:
                beyond.append(pair)
    return alone, inside, beyond


def flat(cell, grid):
    return (cell[0] * grid[1] + cell[1]) * grid[2] + cell[2]


def plans_of(sizes, copies):
    wide = tuple(size + 1 for size in sizes)
    alone, inside, beyond = pair_lists(sizes)

    def places(grid):
        return tuple(
            tuple(float(at) - (size + 1) / 2 for at, size in zip(cell, sizes))
            for cell in itertools.product(*map(range, grid))
        )

    own = list(itertools.product(*map(range, sizes)))
    near = Plan(
        places(sizes),
        (True,) * len(own),
        rounds_of(alone, GROUP) + rounds_of(inside, GROUP),
        False,
        8,
    )
    everywhere = list(itertools.product(*map(range, wide)))
    starters = {pair[0] for pair in beyond}
    far = Plan(
        places(wide),
        tuple(cell in starters for cell in everywhere),
        rounds_of(beyond, GROUP),
        True,
        copies,
    )
    near_table = [tuple(flat(cell, sizes) for cell in pair) for pair in alone + inside]
    far_table = [tuple(flat(cell, wide) for cell in pair) for pair in beyond]
    return (near, near_table), (far, far_table)


def per_device(positions, type_ids, counts, type_charge, type_sigma, type_epsilon):
    size_x, size_y, size_z, width_atoms = positions.shape[1:]
    slots = lax.broadcasted_iota(jnp.int32, type_ids.shape, 3)
    occupied = (slots < counts[..., None]).astype(jnp.float32)
    blank = jnp.zeros(type_ids.shape, jnp.float32)
    atoms = jnp.stack(
        [positions[0], positions[1], positions[2], type_ids.astype(jnp.float32), occupied, blank, blank, blank], 3
    )
    sizes = (size_x, size_y, size_z)
    params = jnp.stack([type_charge, type_sigma, type_epsilon])
    (near, near_table), (far, far_table) = plans_of(sizes, lax.axis_size(ONE))
    own = atoms.reshape((-1, 8, width_atoms))
    extended = jnp.concatenate([atoms, passed_along(atoms[:1], "gx", -1)], 0)
    extended = jnp.concatenate([extended, passed_along(extended[:, :1], GY, -1)], 1)
    own, extended = lax.optimization_barrier((own, extended))
    edge = passed_along(extended[:, :, :1], GZ, -1)
    inner, inner_sums = pair_sums(near, near_table, params, own)
    edge, inner, inner_sums = lax.optimization_barrier((edge, inner, inner_sums))
    extended = jnp.concatenate([extended, edge], 2)
    wide = extended.shape[:3]
    forces, sums = pair_sums(far, far_table, params, extended.reshape((-1, 8, width_atoms)), inner_sums)
    inner = inner.reshape(sizes + (8, width_atoms))[..., :3, :]
    reaction = forces.reshape(wide + (8, width_atoms))[..., :3, :]
    returned = passed_along(reaction[:, :, size_z:], GZ, 1)
    rows = jnp.sum(lax.all_to_all(sums, ONE, 0, 0, tiled=True), 0)
    returned, rows = lax.optimization_barrier((returned, rows))
    reaction = reaction[:, :, :size_z].at[:, :, :1].add(returned)
    returned = passed_along(reaction[:, size_y:], GY, 1)
    copies = jnp.broadcast_to(rows, (lax.axis_size(OTHER), width_atoms))
    summed = jnp.sum(lax.all_to_all(copies, OTHER, 0, 0, tiled=True), 0)[:2]
    reaction = reaction[:, :size_y].at[:, :1].add(returned)
    returned = passed_along(reaction[size_x:], "gx", 1)
    forces = reaction[:size_x].at[:1].add(returned) + inner
    normaliser = 1.0 / (
        size_x
        * lax.axis_size("gx")
        * size_y
        * lax.axis_size(GY)
        * size_z
        * lax.axis_size(GZ)
        * width_atoms
    )
    return (jnp.transpose(forces, (3, 0, 1, 2, 4)), summed * normaliser)


def solution(mesh):
    split = Mesh(
        mesh.devices.reshape(mesh.shape["gx"], 4, 2, 3, 4), ("gx", "gy_0", "gy_1", "gz_0", "gz_1")
    )
    placed = (P(None, "gx", GY, GZ, None), P("gx", GY, GZ, None), P("gx", GY, GZ), P(), P(), P())
    return jax.shard_map(
        per_device,
        mesh=split,
        in_specs=placed,
        out_specs=(P(None, "gx", GY, GZ, None), P()),
        check_vma=False,
    )
```
